32 devices in a mesh: dp: 8 (over y, x, core), section: 4 (over z).
Axes of the slice: x: 2, y: 2, z: 4, core: 2. Of those that a mesh axis runs over, the one named last changes fastest.
Arguments:
- activations: bfloat16 [4, 512, 2048], P(None, 'dp'), may hold values from -6 to 6
- cotangent: bfloat16 [4, 512, 2048], P(None, 'dp'), may hold values from -6 to 6
- weight: bfloat16 [4, 2048, 2048], P('section', 'dp'), may hold values from -0.125 to 0.125
- norm_gain: float32 [4, 2048], P('section'), may hold values from 0.1 to 1.9
- pair_mask: int32 [4, 512, 2048], P('section'), may hold values from 0 to 5, as said below
- earlier_mask: int32 [4, 512, 2048], P('section', 'dp'), may hold values from 0 to 5, as said below
Outputs:
- weight_grad: float32 [4, 2048, 2048], P('section', 'dp')
- flip_count: int32 [4], P('section')
The draws below stay inside these ranges and needn't reach their ends.
Inputs may be any that keep to these rules, and one draw needn't show every extreme that they name: `pair_mask`: pair number of each group of four consecutive rows and each column; pairs numbered (0,1), (0,2), (0,3), (1,2), (1,3), (2,3). `earlier_mask`: pair numbers of the previous step, numbered likewise.
All inputs are finite; a program needn't handle non-finite values.
Results may differ from the reference program's by a relative error of at most 0.02.
Values may be sent and summed in bfloat16 or wider, within the bound.
A program may use at most 64 MiB of HBM per device.

```python
import math
import jax
import jax.numpy as jnp
from jax import lax

D = 2048
MICRO = 4
SECTIONS = 4
BATCH_ROWS = 512
TOKENS = 2048
N_DP = 8


def mask_pair(key):
    base_key = jax.random.fold_in(key, 7301)
    mask_shape = (SECTIONS, D // 4, D)
    current = jax.random.randint(jax.random.fold_in(base_key, 1), mask_shape, 0, 6)
    row_iota = lax.broadcasted_iota(jnp.int32, mask_shape, 1)
    threshold = 100 + 200 * row_iota // (D // 4 - 1)
    dice_rolls = jax.random.randint(jax.random.fold_in(base_key, 2), mask_shape, 0, 1000)
    offsets = jax.random.randint(jax.random.fold_in(base_key, 3), mask_shape, 1, 6)
    earlier = jnp.where(dice_rolls < threshold, (current + offsets) % 6, current)
    return (current.astype(jnp.int32), earlier.astype(jnp.int32))


def draw_pair_mask(key, part):
    return mask_pair(key)[0]


def draw_earlier_mask(key, part):
    return mask_pair(key)[1]


def levels(rng, shape, cuts, smallest, high):
    gain, own = 1.0, jax.random.fold_in(rng, 6)
    for position, blocks in cuts:
        steps = jnp.exp(jax.random.uniform(jax.random.fold_in(own, position), (blocks,), jnp.float32, smallest / len(cuts), high / len(cuts)))
        gain = gain * jnp.repeat(steps, shape[position] // blocks).reshape([-1 if axis == position else 1 for axis in range(len(shape))])
    return gain


def centred(key, extent, width, most, cuts=(), kind=jnp.bfloat16):
    loudness = levels(key, extent, cuts, -0.22, 0.18) if cuts else 1.0
    result = jax.random.normal(key, extent, jnp.float32) * width * loudness
    return jnp.minimum(jnp.maximum(result, -most), most).astype(kind)


def setup_inputs(seed: int = 0) -> dict:
    key_of = jax.random.split(jax.random.key(seed), 7)
    activations = centred(key_of[0], (MICRO, BATCH_ROWS, D), 1.0, 6.0, ((1, 8),))
    cotangent = centred(key_of[1], (MICRO, BATCH_ROWS, D), 1.0, 6.0, ((1, 8),))
    weight = centred(key_of[2], (SECTIONS, D, D), D ** -0.5, 0.125, ((0, 4), (1, 8)))
    norm_gain = jnp.clip(1.0 + 0.18 * jax.random.normal(key_of[3], (SECTIONS, D), jnp.float32), 0.1, 1.9)
    pair_mask = draw_pair_mask(jax.random.fold_in(key_of[6], 71), 0)
    earlier_mask = draw_earlier_mask(jax.random.fold_in(key_of[6], 71), 0)
    return {"activations": activations, "cotangent": cotangent, "weight": weight, "norm_gain": norm_gain, "pair_mask": pair_mask, "earlier_mask": earlier_mask}


epsilon = 1e-06
decay_rate = 4.0
half_root = 0.7071067811865476
density_scale = 0.3989422804014327
first_table = (0, 0, 0, 1, 1, 2)
second_table = (1, 2, 3, 2, 3, 3)

def pair_ends(indices):
    leading = jnp.zeros_like(indices)
    trailing = jnp.zeros_like(indices)
    for pair_index in range(6):
        matches = indices == pair_index
        leading = jnp.where(matches, first_table[pair_index], leading)
        trailing = jnp.where(matches, second_table[pair_index], trailing)
    return (leading, trailing)

def kept_positions(indices):
    leading, trailing = pair_ends(indices)
    groups, columns = indices.shape
    positions = lax.broadcasted_iota(jnp.int32, (groups, 4, columns), 1)
    kept_mask = (positions == leading[:, None, :]) | (positions == trailing[:, None, :])
    return kept_mask.reshape(groups * 4, columns)

def section_forward(inputs, masked, gain_row):
    values = inputs.astype(jnp.float32)
    norm_scale = lax.rsqrt(lax.optimization_barrier(jnp.mean(values * values, axis=-1, keepdims=True)) + epsilon)
    normed = (values * norm_scale * gain_row).astype(jnp.bfloat16)
    preact = jnp.dot(normed, masked, preferred_element_type=jnp.float32)
    normal_cdf = 0.5 * (1.0 + lax.erf(preact * half_root))
    outputs = (values + preact * normal_cdf).astype(jnp.bfloat16)
    return (normed, preact, outputs)

def section_backward(inputs, preact, upstream, masked, gain_row):
    values = inputs.astype(jnp.float32)
    norm_scale = lax.rsqrt(lax.optimization_barrier(jnp.mean(values * values, axis=-1, keepdims=True)) + epsilon)
    normal_cdf = 0.5 * (1.0 + lax.erf(preact * half_root))
    normal_pdf = jnp.exp(-0.5 * preact * preact) * density_scale
    upstream_f = upstream.astype(jnp.float32)
    grad_pre = (upstream_f * (normal_cdf + preact * normal_pdf)).astype(jnp.bfloat16)
    grad_normed = lax.dot_general(grad_pre, masked, (((1,), (1,)), ((), ())), preferred_element_type=jnp.float32)
    scaled_grad = grad_normed * gain_row
    grad_input = norm_scale * scaled_grad - values * norm_scale ** 3 * lax.optimization_barrier(jnp.mean(scaled_grad * values, axis=-1, keepdims=True))
    return (grad_pre, (upstream_f + grad_input).astype(jnp.bfloat16))

def replica_terms(normed, grad_pre, micro_count):
    replicas = N_DP
    model_width = normed.shape[1]
    row_count = normed.shape[0] // (micro_count * replicas)
    normed_split = normed.reshape(micro_count, replicas, row_count, model_width).transpose(1, 0, 2, 3).reshape(replicas, micro_count * row_count, model_width)
    grad_split = grad_pre.reshape(micro_count, replicas, row_count, model_width).transpose(1, 0, 2, 3).reshape(replicas, micro_count * row_count, model_width)

    def add_replica(running, pieces):
        partial_term = lax.dot_general(pieces[0], pieces[1], (((0,), (0,)), ((), ())), preferred_element_type=jnp.float32)
        rounded = lax.optimization_barrier(partial_term.astype(jnp.bfloat16))
        return (running + rounded.astype(jnp.float32), None)
    running, unused = lax.scan(add_replica, jnp.zeros((model_width, model_width), jnp.float32), (normed_split, grad_split))
    return running

def reference(activations, cotangent, weight, norm_gain, pair_mask, earlier_mask):
    micro_count, batch_rows, model_width = activations.shape
    hidden = activations.reshape(micro_count * batch_rows, model_width)
    upstream = cotangent.reshape(micro_count * batch_rows, model_width)
    masked_list = []
    kept_list = []
    for section_index in range(SECTIONS):
        kept_mask = kept_positions(pair_mask[section_index])
        kept_list.append(kept_mask)
        masked_list.append(jnp.where(kept_mask, weight[section_index], jnp.zeros_like(weight[section_index])))
    saved_inputs = []
    saved_normed = []
    saved_preact = []
    for section_index in range(SECTIONS):
        saved_inputs.append(hidden)
        normed, preact, hidden = section_forward(hidden, masked_list[section_index], norm_gain[section_index])
        saved_normed.append(normed)
        saved_preact.append(preact)
    gradients = [None] * SECTIONS
    for section_index in reversed(range(SECTIONS)):
        grad_pre, upstream = section_backward(saved_inputs[section_index], saved_preact[section_index], upstream, masked_list[section_index], norm_gain[section_index])
        dense_part = replica_terms(saved_normed[section_index], grad_pre, micro_count) / math.sqrt(TOKENS)
        decay_part = jnp.where(kept_list[section_index], 0.0, weight[section_index].astype(jnp.float32))
        gradients[section_index] = dense_part + decay_rate * decay_part
    flip_list = []
    for section_index in range(SECTIONS):
        earlier_kept = kept_positions(earlier_mask[section_index])
        flip_list.append(jnp.sum(kept_list[section_index] != earlier_kept).astype(jnp.int32))
    return (jnp.stack(gradients), jnp.stack(flip_list))
```

```python
import functools
import math

import jax
import jax.numpy as jnp
from jax import lax
from jax.experimental import pallas as pl
from jax.experimental.pallas import tpu as pltpu
from jax.sharding import PartitionSpec as P

epsilon = 1e-06
decay_rate = 4.0
half_root = 0.7071067811865476
density_scale = 0.3989422804014327
first_table = (0, 0, 0, 1, 1, 2)
second_table = (1, 2, 3, 2, 3, 3)


def shifted(block, axis, distance):
    devices = range(lax.axis_size(axis))
    route = [(i - distance, i) for i in devices if i - distance in devices]
    return lax.ppermute(block, axis, route)


def pair_ends(indices):
    leading = jnp.zeros_like(indices)
    trailing = jnp.zeros_like(indices)
    for pair_index in range(6):
        matches = indices == pair_index
        leading = jnp.where(matches, first_table[pair_index], leading)
        trailing = jnp.where(matches, second_table[pair_index], trailing)
    return (leading, trailing)


def kept_positions(indices):
    leading, trailing = pair_ends(indices)
    groups, columns = indices.shape
    positions = lax.broadcasted_iota(jnp.int32, (groups, 4, columns), 1)
    kept_mask = (positions == leading[:, None, :]) | (positions == trailing[:, None, :])
    return kept_mask.reshape(groups * 4, columns)


def section_forward(inputs, masked, gain_row):
    values = inputs.astype(jnp.float32)
    norm_scale = lax.rsqrt(jnp.mean(values * values, axis=-1, keepdims=True) + epsilon)
    normed = (values * norm_scale * gain_row).astype(jnp.bfloat16)
    preact = jnp.dot(normed, masked, preferred_element_type=jnp.float32)
    normal_cdf = 0.5 * (1.0 + lax.erf(preact * half_root))
    outputs = (values + preact * normal_cdf).astype(jnp.bfloat16)
    return (normed, preact, outputs)


def section_backward(inputs, preact, upstream, masked, gain_row):
    values = inputs.astype(jnp.float32)
    norm_scale = lax.rsqrt(jnp.mean(values * values, axis=-1, keepdims=True) + epsilon)
    normal_cdf = 0.5 * (1.0 + lax.erf(preact * half_root))
    normal_pdf = jnp.exp(-0.5 * preact * preact) * density_scale
    upstream_f = upstream.astype(jnp.float32)
    grad_pre = (upstream_f * (normal_cdf + preact * normal_pdf)).astype(jnp.bfloat16)
    grad_normed = lax.dot_general(
        grad_pre, masked, (((1,), (1,)), ((), ())), preferred_element_type=jnp.float32
    )
    scaled_grad = grad_normed * gain_row
    grad_input = norm_scale * scaled_grad - values * norm_scale**3 * jnp.mean(
        scaled_grad * values, axis=-1, keepdims=True
    )
    return (grad_pre, (upstream_f + grad_input).astype(jnp.bfloat16))


def write_slot(buffer, new_value, slot_index, is_live):
    old_value = lax.dynamic_index_in_dim(buffer, slot_index, 0, keepdims=False)
    chosen = jnp.where(is_live, new_value, old_value)
    return lax.dynamic_update_index_in_dim(buffer, chosen, slot_index, 0)


def body(activations, cotangent, weight, norm_gain, pair_mask, earlier_mask):
    section_count = lax.axis_size("section")
    replica_count = lax.axis_size("dp")
    section_index = lax.axis_index("section")
    replica_index = lax.axis_index("dp")
    micro_count, row_count, model_width = activations.shape
    shard_rows = weight.shape[1]
    groups = shard_rows // 4
    own_weight = weight[0]
    gain_row = norm_gain[0]
    own_pairs = lax.dynamic_slice_in_dim(pair_mask[0], replica_index * groups, groups, 0)
    own_kept = kept_positions(own_pairs)
    earlier_kept = kept_positions(earlier_mask[0])
    flip_local = jnp.sum(own_kept != earlier_kept).reshape(1)
    flip_sum = lax.psum(flip_local, "dp")
    masked_shard = jnp.where(own_kept, own_weight, jnp.zeros_like(own_weight))
    masked = lax.all_gather(masked_shard, "dp", axis=0, tiled=True)
    tick_count = micro_count + section_count - 1
    act_zeros = jnp.zeros((micro_count, row_count, model_width), jnp.bfloat16)
    stored = (act_zeros,)

    def forward_tick(tick_index, state_tuple):
        received, buffers = state_tuple
        micro_index = tick_index - section_index
        is_live = (micro_index >= 0) & (micro_index < micro_count)
        slot_index = jnp.clip(micro_index, 0, micro_count - 1)
        fresh_rows = lax.dynamic_index_in_dim(activations, slot_index, 0, keepdims=False)
        current = jnp.where(section_index == 0, fresh_rows, received)
        normed, preact, outputs = section_forward(current, masked, gain_row)
        results = (current, normed, preact)
        buffers = tuple(
            (
                write_slot(buffer, update, slot_index, is_live)
                for buffer, update in zip(buffers, results)
            )
        )
        received = shifted(outputs, "section", 1)
        return (received, buffers)

    start_rows = jnp.zeros((row_count, model_width), jnp.bfloat16)
    received, stored = lax.fori_loop(0, tick_count, forward_tick, (start_rows, stored))

    def backward_tick(tick_index, state_tuple):
        received, grad_buffer, normed_buffer = state_tuple
        micro_index = tick_index - (section_count - 1 - section_index)
        is_live = (micro_index >= 0) & (micro_index < micro_count)
        slot_index = jnp.clip(micro_index, 0, micro_count - 1)
        fresh_rows = lax.dynamic_index_in_dim(cotangent, slot_index, 0, keepdims=False)
        upstream = jnp.where(section_index == section_count - 1, fresh_rows, received)
        inputs = lax.dynamic_index_in_dim(stored[0], slot_index, 0, keepdims=False)
        normed, preact, unused = section_forward(inputs, masked, gain_row)
        normed_buffer = write_slot(normed_buffer, normed, slot_index, is_live)
        grad_pre, grad_input = section_backward(inputs, preact, upstream, masked, gain_row)
        grad_buffer = write_slot(grad_buffer, grad_pre, slot_index, is_live)
        received = shifted(grad_input, "section", -1)
        return (received, grad_buffer, normed_buffer)

    received, grad_buffer, normed_buffer = lax.fori_loop(
        0, tick_count, backward_tick, (start_rows, act_zeros, act_zeros)
    )
    flat_normed = normed_buffer.reshape(micro_count * row_count, model_width)
    flat_grad = grad_buffer.reshape(micro_count * row_count, model_width)
    summed = lax.psum_scatter(
        lax.dot_general(
            flat_normed, flat_grad, (((0,), (0,)), ((), ())), preferred_element_type=jnp.float32
        ).astype(jnp.bfloat16),
        "dp",
        scatter_dimension=0,
        tiled=True,
    ).astype(jnp.float32)
    token_total = micro_count * row_count * replica_count
    dense_part = summed / math.sqrt(token_total)
    decay_part = jnp.where(own_kept, 0.0, own_weight.astype(jnp.float32))
    gradient = dense_part + decay_rate * decay_part
    return (gradient[None], flip_sum)


def pick_chunk(rows):
    return 32 if rows % 32 == 0 else 16


def fused_fits(mesh, activations, weight):
    replicas, sections = mesh.shape["dp"], mesh.shape["section"]
    micro, batch, width = activations.shape
    shard_rows = weight.shape[1] // replicas
    rows = micro * batch // replicas
    gathered = replicas // 2 * rows * width * 2
    return (
        replicas % 2 == 0
        and replicas > 2
        and sections > 1
        and shard_rows % 128 == 0
        and rows % 16 == 0
        and width % 512 == 0
        and gathered + 3 * width * width * 2 < 40 * 2**20
    )


def spread_matrix(count, transposed):
    groups = count // 4
    rows = lax.broadcasted_iota(jnp.int32, (count, count), 1 if transposed else 0)
    columns = lax.broadcasted_iota(jnp.int32, (count, count), 0 if transposed else 1)
    place = sum((columns >= groups * j).astype(jnp.int32) for j in (1, 2, 3))
    hit = rows == 4 * (columns - groups * place) + place
    return jnp.where(hit, 1.0, 0.0).astype(jnp.bfloat16)


def fused_kernel(
    chunk, tokens, act, cot, weight, gain, pairs, earlier, out, flips,
    packed, full, hidden, normed, deriv, outgoing, upstream, downstream, grads, terms,
    scaled, partial, incoming, counts,
    pack_send, pack_recv, relay_send, relay_recv, fwd_send, fwd_recv, bwd_send, bwd_recv,
    term_send, term_recv, grad_send, grad_recv, part_send, part_recv, flip_send, flip_recv, pair_sem,
):
    section = lax.axis_index("section")
    sections = lax.axis_size("section")
    me = lax.axis_index("dp")
    chips = lax.axis_size("dp") // 2
    chip = lax.div(me, 2)
    core = lax.rem(me, 2)
    sibling = 2 * chip + 1 - core
    last = sections - 1
    shard_rows, width = weight.shape
    groups = shard_rows // 4
    rows = hidden.shape[0]
    steps = rows // chunk
    tile = 512
    tiles = width // tile
    own_columns = pl.multiple_of(chip * 2 * shard_rows, 2 * shard_rows)

    def peer_chip(k):
        return lax.rem(chip + k, chips)

    def at_dp(index):
        return {"dp": index}

    def remote(src, dst, send, recv, where):
        return pltpu.make_async_remote_copy(
            src_ref=src, dst_ref=dst, send_sem=send, recv_sem=recv,
            device_id=where, device_id_type=pl.DeviceIdType.MESH,
        )

    barrier = pltpu.get_barrier_semaphore()

    def greet(where):
        pl.semaphore_signal(barrier, inc=1, device_id=where, device_id_type=pl.DeviceIdType.MESH)

    for k in range(1, chips):
        greet(at_dp(2 * peer_chip(k) + core))
    greet(at_dp(sibling))

    @pl.when(section > 0)
    def _():
        greet({"section": section - 1})

    @pl.when(section < last)
    def _():
        greet({"section": section + 1})

    own_pairs = pairs.at[pl.ds(pl.multiple_of(me * groups, groups), groups), :]
    gather_rows = spread_matrix(shard_rows, True)
    for t in range(tiles):
        cols = slice(t * tile, (t + 1) * tile)
        split = jnp.dot(gather_rows, weight[:, cols], preferred_element_type=jnp.float32)
        w0, w1, w2, w3 = (split[j * groups:(j + 1) * groups] for j in range(4))
        p = own_pairs[:, cols]
        first = jnp.where(p <= 2, w0, jnp.where(p <= 4, w1, w2))
        second = jnp.where(p == 0, w1, jnp.where((p == 1) | (p == 3), w2, w3))
        packed[me, 0:groups, cols] = first.astype(jnp.bfloat16)
        packed[me, groups:2 * groups, cols] = second.astype(jnp.bfloat16)

    pl.semaphore_wait(barrier, chips + (section > 0).astype(jnp.int32) + (section < last).astype(jnp.int32))

    def pack_copy(k, source):
        slot = packed.at[2 * source + core]
        return remote(slot, slot, pack_send.at[k], pack_recv.at[source], at_dp(2 * peer_chip(k) + core))

    def relay_copy(source, parity):
        slot = packed.at[2 * source + parity]
        return remote(slot, slot, relay_send.at[source], relay_recv.at[source], at_dp(sibling))

    for k in range(1, chips):
        pack_copy(k, chip).start()
    relay_copy(chip, core).start()

    p = own_pairs[...]
    q = earlier[...]
    changed = jnp.where(p == q, 0, jnp.where(p + q == 5, 4, 2))
    total = jnp.zeros((8, 128), jnp.int32)
    for a in range(groups // 8):
        for b in range(width // 128):
            total = total + changed[a * 8:(a + 1) * 8, b * 128:(b + 1) * 128]
    counts[chip] = total

    def flip_copy(k, source):
        slot = counts.at[source]
        return remote(slot, slot, flip_send.at[k], flip_recv.at[source], at_dp(2 * peer_chip(k) + core))

    for k in range(1, chips):
        flip_copy(k, chip).start()

    spread_rows = spread_matrix(shard_rows, False)

    def unpack(owner):
        owned = pl.multiple_of(owner * groups, groups)
        target = pl.multiple_of(owner * shard_rows, shard_rows)
        for t in range(tiles):
            cols = slice(t * tile, (t + 1) * tile)
            p = pairs[pl.ds(owned, groups), cols]
            v0 = packed[owner, 0:groups, cols].astype(jnp.float32)
            v1 = packed[owner, groups:2 * groups, cols].astype(jnp.float32)
            zero = jnp.zeros_like(v0)
            parts = (
                jnp.where(p <= 2, v0, zero),
                jnp.where((p == 3) | (p == 4), v0, jnp.where(p == 0, v1, zero)),
                jnp.where(p == 5, v0, jnp.where((p == 1) | (p == 3), v1, zero)),
                jnp.where((p == 2) | (p >= 4), v1, zero),
            )
            stacked = jnp.concatenate(parts, axis=0).astype(jnp.bfloat16)
            spread = jnp.dot(spread_rows, stacked, preferred_element_type=jnp.float32)
            full[pl.ds(target, shard_rows), cols] = spread.astype(jnp.bfloat16)

    def receive(k, carry):
        source = lax.rem(chip + k, chips)

        @pl.when(k > 0)
        def _():
            pack_copy(1, source).wait_recv()
            relay_copy(source, core).start()

        unpack(2 * source + core)
        relay_copy(source, 1 - core).wait_recv()
        unpack(2 * source + 1 - core)
        return carry

    lax.fori_loop(0, chips, receive, 0)

    @pl.when(section == 0)
    def _():
        for m in range(act.shape[0]):
            hidden[m * act.shape[1]:(m + 1) * act.shape[1], :] = act[m]

    @pl.when(section == last)
    def _():
        for m in range(cot.shape[0]):
            upstream[m * cot.shape[1]:(m + 1) * cot.shape[1], :] = cot[m]

    def span(i):
        return pl.ds(pl.multiple_of(i * chunk, chunk), chunk)

    def fwd_copy(i):
        return remote(outgoing.at[span(i)], hidden.at[span(i)], fwd_send.at[i], fwd_recv.at[i], {"section": section + 1})

    def fwd_arrival(i):
        return remote(outgoing.at[span(i)], hidden.at[span(i)], fwd_send.at[i], fwd_recv.at[i], {"section": section})

    def bwd_copy(i):
        return remote(downstream.at[span(i)], upstream.at[span(i)], bwd_send.at[i], bwd_recv.at[i], {"section": section - 1})

    def bwd_arrival(i):
        return remote(downstream.at[span(i)], upstream.at[span(i)], bwd_send.at[i], bwd_recv.at[i], {"section": section})

    def term_copy(k, i):
        peer = peer_chip(k)
        wanted = pl.ds(pl.multiple_of(peer * 2 * shard_rows, 2 * shard_rows), 2 * shard_rows)
        return remote(
            normed.at[span(i), wanted], terms.at[chip, span(i)],
            term_send.at[k, i], term_recv.at[chip, i], at_dp(2 * peer + core),
        )

    def grad_copy(k, i):
        return remote(
            grads.at[chip, span(i)], grads.at[chip, span(i)],
            grad_send.at[k, i], grad_recv.at[chip, i], at_dp(2 * peer_chip(k) + core),
        )

    def forward(i):
        @pl.when(section > 0)
        def _():
            fwd_arrival(i).wait_recv()

        values = hidden[span(i)].astype(jnp.float32)
        scale = lax.rsqrt(jnp.mean(values * values, axis=-1, keepdims=True) + epsilon)
        rounded = (values * scale * gain[...]).astype(jnp.bfloat16)
        normed[span(i)] = rounded
        for t in range(tiles):
            cols = slice(t * tile, (t + 1) * tile)
            preact = jnp.dot(rounded, full[:, cols], preferred_element_type=jnp.float32)
            cdf = 0.5 * (1.0 + lax.erf(preact * half_root))
            pdf = jnp.exp(-0.5 * preact * preact) * density_scale
            deriv[span(i), cols] = cdf + preact * pdf
            outgoing[span(i), cols] = (values[:, cols] + preact * cdf).astype(jnp.bfloat16)

        @pl.when(section < last)
        def _():
            fwd_copy(i).start()

        terms[chip, span(i)] = normed[span(i), pl.ds(own_columns, 2 * shard_rows)]
        for k in range(1, chips):
            term_copy(k, i).start()

    def backward(i):
        @pl.when(section < last)
        def _():
            bwd_arrival(i).wait_recv()

        above = upstream[span(i)].astype(jnp.float32)
        grad_pre = (above * deriv[span(i)]).astype(jnp.bfloat16)
        grads[chip, span(i)] = grad_pre
        for k in range(1, chips):
            grad_copy(k, i).start()

        @pl.when(section > 0)
        def _():
            values = hidden[span(i)].astype(jnp.float32)
            scale = lax.rsqrt(jnp.mean(values * values, axis=-1, keepdims=True) + epsilon)
            along = jnp.zeros((chunk, 1), jnp.float32)
            for t in range(tiles):
                cols = slice(t * tile, (t + 1) * tile)
                piece = lax.dot_general(
                    grad_pre, full[cols, :], (((1,), (1,)), ((), ())), preferred_element_type=jnp.float32
                ) * gain[:, cols]
                scaled[:, cols] = piece
                along = along + jnp.sum(piece * values[:, cols], axis=-1, keepdims=True)
            pull = scale * scale * scale * (along / width)
            result = upstream[span(i)].astype(jnp.float32) + scale * scaled[...] - values * pull
            downstream[span(i)] = result.astype(jnp.bfloat16)
            bwd_copy(i).start()

    def step(k, carry):
        at_last = (section == last).astype(jnp.int32)
        half = lax.div(k, 2)
        goes_back = at_last * lax.rem(k, 2) + (1 - at_last) * lax.div(k, steps)
        index = at_last * half + (1 - at_last) * lax.rem(k, steps)

        @pl.when(goes_back == 0)
        def _():
            forward(index)

        @pl.when(goes_back == 1)
        def _():
            backward(index)

        return carry

    lax.fori_loop(0, 2 * steps, step, 0)

    def arrivals(i, carry):
        for k in range(1, chips):
            source = peer_chip(k)
            remote(
                terms.at[source, span(i)], terms.at[source, span(i)],
                term_send.at[k, i], term_recv.at[source, i], at_dp(me),
            ).wait_recv()
            remote(
                grads.at[source, span(i)], grads.at[source, span(i)],
                grad_send.at[k, i], grad_recv.at[source, i], at_dp(me),
            ).wait_recv()
        return carry

    lax.fori_loop(0, steps, arrivals, 0)

    def product(half, cols):
        left = pl.ds(pl.multiple_of(half * shard_rows, shard_rows), shard_rows)
        total = jnp.zeros((shard_rows, tile), jnp.float32)
        for c in range(chips):
            total = total + lax.dot_general(
                terms[c, :, left], grads[c, :, cols], (((0,), (0,)), ((), ())), preferred_element_type=jnp.float32
            )
        return total

    def part_copy(t):
        return remote(partial.at[t], incoming.at[t], part_send.at[t], part_recv.at[t], at_dp(sibling))

    for t in range(tiles):
        partial[t] = product(1 - core, slice(t * tile, (t + 1) * tile)).astype(jnp.bfloat16)
        part_copy(t).start()
    own_rows = pl.ds(pl.multiple_of(me * shard_rows, shard_rows), shard_rows)
    for t in range(tiles):
        cols = slice(t * tile, (t + 1) * tile)
        pruned = weight[:, cols].astype(jnp.float32) - full[own_rows, cols].astype(jnp.float32)
        out[:, cols] = product(core, cols) * (1.0 / math.sqrt(tokens)) + decay_rate * pruned

    for k in range(1, chips):
        flip_copy(k, peer_chip(k)).wait_recv()
    total = counts[0]
    for c in range(1, chips):
        total = total + counts[c]
    counts[chips] = total
    pair_copy = remote(counts.at[chips], counts.at[chips + 1], pair_sem.at[0], pair_sem.at[1], at_dp(sibling))
    pair_copy.start()

    for t in range(tiles):
        cols = slice(t * tile, (t + 1) * tile)
        part_copy(t).wait_recv()
        out[:, cols] = out[:, cols] + incoming[t].astype(jnp.float32) * (1.0 / math.sqrt(tokens))
    pair_copy.wait_recv()
    flips[...] = counts[chips] + counts[chips + 1]

    pair_copy.wait_send()
    for t in range(tiles):
        part_copy(t).wait_send()
    for k in range(1, chips):
        pack_copy(k, chip).wait_send()
        flip_copy(k, chip).wait_send()

    for c in range(chips):
        relay_copy(c, core).wait_send()

    def drain(i, carry):
        for k in range(1, chips):
            term_copy(k, i).wait_send()
            grad_copy(k, i).wait_send()

        @pl.when(section < last)
        def _():
            fwd_copy(i).wait_send()

        @pl.when(section > 0)
        def _():
            bwd_copy(i).wait_send()

        return carry

    lax.fori_loop(0, steps, drain, 0)


def fused_body(activations, cotangent, weight, norm_gain, pair_mask, earlier_mask):
    replicas = lax.axis_size("dp")
    chips = replicas // 2
    micro, micro_rows, width = activations.shape
    shard_rows = weight.shape[1]
    groups = shard_rows // 4
    rows = micro * micro_rows
    chunk = pick_chunk(rows)
    steps = rows // chunk
    tile = 512
    tiles = width // tile
    bf, f32 = jnp.bfloat16, jnp.float32
    dma = pltpu.SemaphoreType.DMA
    vmem = pl.BlockSpec(memory_space=pltpu.VMEM)
    gradient, flips = pl.pallas_call(
        functools.partial(fused_kernel, chunk, rows * replicas),
        out_shape=(
            jax.ShapeDtypeStruct((shard_rows, width), f32),
            jax.ShapeDtypeStruct((8, 128), jnp.int32),
        ),
        in_specs=[vmem] * 6,
        out_specs=(vmem, vmem),
        scratch_shapes=[
            pltpu.VMEM((replicas, 2 * groups, width), bf),
            pltpu.VMEM((width, width), bf),
            pltpu.VMEM((rows, width), bf),
            pltpu.VMEM((rows, width), bf),
            pltpu.VMEM((rows, width), f32),
            pltpu.VMEM((rows, width), bf),
            pltpu.VMEM((rows, width), bf),
            pltpu.VMEM((rows, width), bf),
            pltpu.VMEM((chips, rows, width), bf),
            pltpu.VMEM((chips, rows, 2 * shard_rows), bf),
            pltpu.VMEM((chunk, width), f32),
            pltpu.VMEM((tiles, shard_rows, tile), bf),
            pltpu.VMEM((tiles, shard_rows, tile), bf),
            pltpu.VMEM((chips + 2, 8, 128), jnp.int32),
            dma((chips,)), dma((chips,)), dma((chips,)), dma((chips,)),
            dma((steps,)), dma((steps,)), dma((steps,)), dma((steps,)),
            dma((chips, steps)), dma((chips, steps)), dma((chips, steps)), dma((chips, steps)),
            dma((tiles,)), dma((tiles,)), dma((chips,)), dma((chips,)), dma((2,)),
        ],
        compiler_params=pltpu.CompilerParams(
            collective_id=0, has_side_effects=True, vmem_limit_bytes=60 * 2**20
        ),
        name="fused_step",
    )(
        activations, cotangent, weight[0], norm_gain, pair_mask[0], earlier_mask[0],
    )
    return (gradient[None], jnp.sum(flips).reshape(1))


def solution(mesh):
    placed = (
        P(None, "dp", None),
        P(None, "dp", None),
        P("section", "dp", None),
        P("section", None),
        P("section", None, None),
        P("section", "dp", None),
    )

    def step(*arrays):
        chosen = fused_body if fused_fits(mesh, arrays[0], arrays[2]) else body
        return jax.shard_map(
            chosen,
            mesh=mesh,
            in_specs=placed,
            out_specs=(P("section", "dp", None), P("section")),
            check_vma=False,
        )(*arrays)

    return step
```

```python
import functools
import math

import jax
import jax.numpy as jnp
from jax import lax
from jax.experimental import pallas as pl
from jax.experimental.pallas import tpu as pltpu
from jax.sharding import PartitionSpec as P

epsilon = 1e-06
decay_rate = 4.0
half_root = 0.7071067811865476
density_scale = 0.3989422804014327
first_table = (0, 0, 0, 1, 1, 2)
second_table = (1, 2, 3, 2, 3, 3)


def shifted(block, axis, distance):
    devices = range(lax.axis_size(axis))
    route = [(i - distance, i) for i in devices if i - distance in devices]
    return lax.ppermute(block, axis, route)


def pair_ends(indices):
    leading = jnp.zeros_like(indices)
    trailing = jnp.zeros_like(indices)
    for pair_index in range(6):
        matches = indices == pair_index
        leading = jnp.where(matches, first_table[pair_index], leading)
        trailing = jnp.where(matches, second_table[pair_index], trailing)
    return (leading, trailing)


def kept_positions(indices):
    leading, trailing = pair_ends(indices)
    groups, columns = indices.shape
    positions = lax.broadcasted_iota(jnp.int32, (groups, 4, columns), 1)
    kept_mask = (positions == leading[:, None, :]) | (positions == trailing[:, None, :])
    return kept_mask.reshape(groups * 4, columns)


def section_forward(inputs, masked, gain_row):
    values = inputs.astype(jnp.float32)
    norm_scale = lax.rsqrt(jnp.mean(values * values, axis=-1, keepdims=True) + epsilon)
    normed = (values * norm_scale * gain_row).astype(jnp.bfloat16)
    preact = jnp.dot(normed, masked, preferred_element_type=jnp.float32)
    normal_cdf = 0.5 * (1.0 + lax.erf(preact * half_root))
    outputs = (values + preact * normal_cdf).astype(jnp.bfloat16)
    return (normed, preact, outputs)


def section_backward(inputs, preact, upstream, masked, gain_row):
    values = inputs.astype(jnp.float32)
    norm_scale = lax.rsqrt(jnp.mean(values * values, axis=-1, keepdims=True) + epsilon)
    normal_cdf = 0.5 * (1.0 + lax.erf(preact * half_root))
    normal_pdf = jnp.exp(-0.5 * preact * preact) * density_scale
    upstream_f = upstream.astype(jnp.float32)
    grad_pre = (upstream_f * (normal_cdf + preact * normal_pdf)).astype(jnp.bfloat16)
    grad_normed = lax.dot_general(
        grad_pre, masked, (((1,), (1,)), ((), ())), preferred_element_type=jnp.float32
    )
    scaled_grad = grad_normed * gain_row
    grad_input = norm_scale * scaled_grad - values * norm_scale**3 * jnp.mean(
        scaled_grad * values, axis=-1, keepdims=True
    )
    return (grad_pre, (upstream_f + grad_input).astype(jnp.bfloat16))


def write_slot(buffer, new_value, slot_index, is_live):
    old_value = lax.dynamic_index_in_dim(buffer, slot_index, 0, keepdims=False)
    chosen = jnp.where(is_live, new_value, old_value)
    return lax.dynamic_update_index_in_dim(buffer, chosen, slot_index, 0)


def body(activations, cotangent, weight, norm_gain, pair_mask, earlier_mask):
    section_count = lax.axis_size("section")
    replica_count = lax.axis_size("dp")
    section_index = lax.axis_index("section")
    replica_index = lax.axis_index("dp")
    micro_count, row_count, model_width = activations.shape
    shard_rows = weight.shape[1]
    groups = shard_rows // 4
    own_weight = weight[0]
    gain_row = norm_gain[0]
    own_pairs = lax.dynamic_slice_in_dim(pair_mask[0], replica_index * groups, groups, 0)
    own_kept = kept_positions(own_pairs)
    earlier_kept = kept_positions(earlier_mask[0])
    flip_local = jnp.sum(own_kept != earlier_kept).reshape(1)
    flip_sum = lax.psum(flip_local, "dp")
    masked_shard = jnp.where(own_kept, own_weight, jnp.zeros_like(own_weight))
    masked = lax.all_gather(masked_shard, "dp", axis=0, tiled=True)
    tick_count = micro_count + section_count - 1
    act_zeros = jnp.zeros((micro_count, row_count, model_width), jnp.bfloat16)
    stored = (act_zeros,)

    def forward_tick(tick_index, state_tuple):
        received, buffers = state_tuple
        micro_index = tick_index - section_index
        is_live = (micro_index >= 0) & (micro_index < micro_count)
        slot_index = jnp.clip(micro_index, 0, micro_count - 1)
        fresh_rows = lax.dynamic_index_in_dim(activations, slot_index, 0, keepdims=False)
        current = jnp.where(section_index == 0, fresh_rows, received)
        normed, preact, outputs = section_forward(current, masked, gain_row)
        results = (current, normed, preact)
        buffers = tuple(
            (
                write_slot(buffer, update, slot_index, is_live)
                for buffer, update in zip(buffers, results)
            )
        )
        received = shifted(outputs, "section", 1)
        return (received, buffers)

    start_rows = jnp.zeros((row_count, model_width), jnp.bfloat16)
    received, stored = lax.fori_loop(0, tick_count, forward_tick, (start_rows, stored))

    def backward_tick(tick_index, state_tuple):
        received, grad_buffer, normed_buffer = state_tuple
        micro_index = tick_index - (section_count - 1 - section_index)
        is_live = (micro_index >= 0) & (micro_index < micro_count)
        slot_index = jnp.clip(micro_index, 0, micro_count - 1)
        fresh_rows = lax.dynamic_index_in_dim(cotangent, slot_index, 0, keepdims=False)
        upstream = jnp.where(section_index == section_count - 1, fresh_rows, received)
        inputs = lax.dynamic_index_in_dim(stored[0], slot_index, 0, keepdims=False)
        normed, preact, unused = section_forward(inputs, masked, gain_row)
        normed_buffer = write_slot(normed_buffer, normed, slot_index, is_live)
        grad_pre, grad_input = section_backward(inputs, preact, upstream, masked, gain_row)
        grad_buffer = write_slot(grad_buffer, grad_pre, slot_index, is_live)
        received = shifted(grad_input, "section", -1)
        return (received, grad_buffer, normed_buffer)

    received, grad_buffer, normed_buffer = lax.fori_loop(
        0, tick_count, backward_tick, (start_rows, act_zeros, act_zeros)
    )
    flat_normed = normed_buffer.reshape(micro_count * row_count, model_width)
    flat_grad = grad_buffer.reshape(micro_count * row_count, model_width)
    summed = lax.psum_scatter(
        lax.dot_general(
            flat_normed, flat_grad, (((0,), (0,)), ((), ())), preferred_element_type=jnp.float32
        ).astype(jnp.bfloat16),
        "dp",
        scatter_dimension=0,
        tiled=True,
    ).astype(jnp.float32)
    token_total = micro_count * row_count * replica_count
    dense_part = summed / math.sqrt(token_total)
    decay_part = jnp.where(own_kept, 0.0, own_weight.astype(jnp.float32))
    gradient = dense_part + decay_rate * decay_part
    return (gradient[None], flip_sum)


HALVES = (0, 1)


def pick_chunk(rows):
    return 32 if rows % 32 == 0 else 16


def fused_fits(mesh, activations, weight):
    replicas, sections = mesh.shape["dp"], mesh.shape["section"]
    micro, batch, width = activations.shape
    shard_rows = weight.shape[1] // replicas
    rows = micro * batch // replicas
    gathered = replicas // 2 * rows * width * 2
    return (
        replicas % 2 == 0
        and replicas == 2 * len(HALVES) ** 2
        and sections > 1
        and shard_rows % 128 == 0
        and rows % 16 == 0
        and width % 512 == 0
        and gathered + 3 * width * width * 2 < 40 * 2**20
    )


def spread_matrix(count, transposed):
    groups = count // 4
    rows = lax.broadcasted_iota(jnp.int32, (count, count), 1 if transposed else 0)
    columns = lax.broadcasted_iota(jnp.int32, (count, count), 0 if transposed else 1)
    place = sum((columns >= groups * j).astype(jnp.int32) for j in (1, 2, 3))
    hit = rows == 4 * (columns - groups * place) + place
    return jnp.where(hit, 1.0, 0.0).astype(jnp.bfloat16)


def fused_kernel(
    chunk, tokens, act, cot, weight, gain, pairs_hbm, earlier, out, flips,
    packed, full, hidden, normed, deriv, outgoing, upstream, downstream, grads, terms,
    scaled, partial, incoming, counts, pairs, own_pairs, load_sem, row_sem,
    pack_send, pack_recv, relay_send, relay_recv, fwd_send, fwd_recv, bwd_send, bwd_recv,
    term_send, term_recv, grad_send, grad_recv, part_send, part_recv, flip_send, flip_recv, pair_sem,
):
    section = lax.axis_index("section")
    sections = lax.axis_size("section")
    me = lax.axis_index("dp")
    chips = lax.axis_size("dp") // 2
    chip = lax.div(me, 2)
    core = lax.rem(me, 2)
    sibling = 2 * chip + 1 - core
    last = sections - 1
    shard_rows, width = weight.shape
    groups = shard_rows // 4
    rows = hidden.shape[0]
    steps = rows // chunk
    tile = 512
    tiles = width // tile
    across = chip + 1 - 2 * lax.rem(chip, 2)
    along_y = lax.rem(chip + 2, chips)
    corner = lax.rem(across + 2, chips)
    near = (across, along_y)
    own_columns = pl.multiple_of(chip * 2 * shard_rows, 2 * shard_rows)

    def peer_chip(k):
        return lax.rem(chip + k, chips)

    def at_dp(index):
        return {"dp": index}

    def remote(src, dst, send, recv, where):
        return pltpu.make_async_remote_copy(
            src_ref=src, dst_ref=dst, send_sem=send, recv_sem=recv,
            device_id=where, device_id_type=pl.DeviceIdType.MESH,
        )

    barrier = pltpu.get_barrier_semaphore()

    def greet(where):
        pl.semaphore_signal(barrier, inc=1, device_id=where, device_id_type=pl.DeviceIdType.MESH)

    for k in range(1, chips):
        greet(at_dp(2 * peer_chip(k) + core))
    greet(at_dp(sibling))

    @pl.when(section > 0)
    def _():
        greet({"section": section - 1})

    @pl.when(section < last)
    def _():
        greet({"section": section + 1})

    own_load = pltpu.make_async_copy(
        pairs_hbm.at[pl.ds(pl.multiple_of(me * groups, groups), groups), :], own_pairs, load_sem.at[0]
    )
    own_load.start()
    all_load = pltpu.make_async_copy(pairs_hbm, pairs, load_sem.at[1])
    all_load.start()
    micro_rows = act.shape[1]

    def row_loads(source, target):
        return [
            pltpu.make_async_copy(source.at[m], target.at[pl.ds(m * micro_rows, micro_rows)], row_sem.at[m])
            for m in range(act.shape[0])
        ]

    @pl.when(section == 0)
    def _():
        for load in row_loads(act, hidden):
            load.start()

    @pl.when(section == last)
    def _():
        for load in row_loads(cot, upstream):
            load.start()

    own_load.wait()
    gather_rows = spread_matrix(shard_rows, True)
    for t in range(tiles):
        cols = slice(t * tile, (t + 1) * tile)
        split = jnp.dot(gather_rows, weight[:, cols], preferred_element_type=jnp.float32)
        w0, w1, w2, w3 = (split[j * groups:(j + 1) * groups] for j in range(4))
        p = own_pairs[:, cols]
        first = jnp.where(p <= 2, w0, jnp.where(p <= 4, w1, w2))
        second = jnp.where(p == 0, w1, jnp.where((p == 1) | (p == 3), w2, w3))
        packed[me, 0:groups, cols] = first.astype(jnp.bfloat16)
        packed[me, groups:2 * groups, cols] = second.astype(jnp.bfloat16)

    pl.semaphore_wait(barrier, chips + (section > 0).astype(jnp.int32) + (section < last).astype(jnp.int32))

    def half_rows(h):
        return pl.ds(h * groups, groups)

    def pack_copy(way, source, h, route):
        slot = packed.at[2 * source + core, half_rows(h)]
        return remote(slot, slot, pack_send.at[route, h], pack_recv.at[source, h], at_dp(2 * near[way] + core))

    def pack_own(way, h):
        return pack_copy(way, chip, h, way)

    def pack_onward(way):
        return pack_copy(1 - way, near[way], way, 2)

    def pack_arrival(source, h):
        return pack_copy(0, source, h, 0)

    def relay_copy(source, parity):
        slot = packed.at[2 * source + parity]
        return remote(slot, slot, relay_send.at[source], relay_recv.at[source], at_dp(sibling))

    for h in HALVES:
        for way in (0, 1):
            pack_own(way, h if way == 0 else 1 - h).start()
    relay_copy(chip, core).start()

    p = own_pairs[...]
    q = earlier[...]
    changed = jnp.where(p == q, 0, jnp.where(p + q == 5, 4, 2))
    total = jnp.zeros((8, 128), jnp.int32)
    for a in range(groups // 8):
        for b in range(width // 128):
            total = total + changed[a * 8:(a + 1) * 8, b * 128:(b + 1) * 128]
    counts[chip] = total

    def flip_copy(k, source):
        slot = counts.at[source]
        return remote(slot, slot, flip_send.at[k], flip_recv.at[source], at_dp(2 * peer_chip(k) + core))

    for k in range(1, chips):
        flip_copy(k, chip).start()

    spread_rows = spread_matrix(shard_rows, False)

    def unpack(owner):
        owned = pl.multiple_of(owner * groups, groups)
        target = pl.multiple_of(owner * shard_rows, shard_rows)
        for t in range(tiles):
            cols = slice(t * tile, (t + 1) * tile)
            p = pairs[pl.ds(owned, groups), cols]
            v0 = packed[owner, 0:groups, cols].astype(jnp.float32)
            v1 = packed[owner, groups:2 * groups, cols].astype(jnp.float32)
            zero = jnp.zeros_like(v0)
            parts = (
                jnp.where(p <= 2, v0, zero),
                jnp.where((p == 3) | (p == 4), v0, jnp.where(p == 0, v1, zero)),
                jnp.where(p == 5, v0, jnp.where((p == 1) | (p == 3), v1, zero)),
                jnp.where((p == 2) | (p >= 4), v1, zero),
            )
            stacked = jnp.concatenate(parts, axis=0).astype(jnp.bfloat16)
            spread = jnp.dot(spread_rows, stacked, preferred_element_type=jnp.float32)
            full[pl.ds(target, shard_rows), cols] = spread.astype(jnp.bfloat16)

    all_load.wait()

    def unpack_two(first, second):
        def one(k, carry):
            unpack(jnp.where(k == 0, first, second))
            return carry

        lax.fori_loop(0, 2, one, 0)

    relay_copy(chip, 1 - core).wait_recv()
    unpack_two(2 * chip + core, 2 * chip + 1 - core)
    for way in (0, 1):
        pack_arrival(near[way], way).wait_recv()
        pack_onward(way).start()
    for way in (0, 1):
        pack_arrival(near[way], 1 - way).wait_recv()
        relay_copy(near[way], core).start()
    unpack_two(2 * across + core, 2 * along_y + core)
    for way in (0, 1):
        relay_copy(near[way], 1 - core).wait_recv()
    unpack_two(2 * across + 1 - core, 2 * along_y + 1 - core)
    for h in HALVES:
        pack_arrival(corner, h).wait_recv()
    relay_copy(corner, core).start()
    unpack_two_first = 2 * corner + core
    relay_copy(corner, 1 - core).wait_recv()
    unpack_two(unpack_two_first, 2 * corner + 1 - core)

    @pl.when(section == 0)
    def _():
        for load in row_loads(act, hidden):
            load.wait()

    @pl.when(section == last)
    def _():
        for load in row_loads(cot, upstream):
            load.wait()

    def span(i):
        return pl.ds(pl.multiple_of(i * chunk, chunk), chunk)

    def fwd_copy(i):
        return remote(outgoing.at[span(i)], hidden.at[span(i)], fwd_send.at[i], fwd_recv.at[i], {"section": section + 1})

    def fwd_arrival(i):
        return remote(outgoing.at[span(i)], hidden.at[span(i)], fwd_send.at[i], fwd_recv.at[i], {"section": section})

    def bwd_copy(i):
        return remote(downstream.at[span(i)], upstream.at[span(i)], bwd_send.at[i], bwd_recv.at[i], {"section": section - 1})

    def bwd_arrival(i):
        return remote(downstream.at[span(i)], upstream.at[span(i)], bwd_send.at[i], bwd_recv.at[i], {"section": section})

    def term_copy(k, i):
        peer = peer_chip(k)
        wanted = pl.ds(pl.multiple_of(peer * 2 * shard_rows, 2 * shard_rows), 2 * shard_rows)
        return remote(
            normed.at[span(i), wanted], terms.at[chip, span(i)],
            term_send.at[k, i], term_recv.at[chip, i], at_dp(2 * peer + core),
        )

    def grad_copy(way, source, h, route, i):
        slot = grads.at[source, span(i), pl.ds(h * (width // 2), width // 2)]
        return remote(
            slot, slot, grad_send.at[route * 2 + h, i], grad_recv.at[source * 2 + h, i], at_dp(2 * near[way] + core)
        )

    def grad_own(way, h, i):
        return grad_copy(way, chip, h, way, i)

    def grad_onward(way, i):
        return grad_copy(1 - way, near[way], way, 2, i)

    def grad_arrival(source, h, i):
        return grad_copy(0, source, h, 0, i)

    def pass_on(i):
        for way in (0, 1):
            grad_arrival(near[way], way, i).wait_recv()
            grad_onward(way, i).start()

    def forward(i):
        @pl.when(section > 0)
        def _():
            fwd_arrival(i).wait_recv()

        values = hidden[span(i)].astype(jnp.float32)
        scale = lax.rsqrt(jnp.mean(values * values, axis=-1, keepdims=True) + epsilon)
        rounded = (values * scale * gain[...]).astype(jnp.bfloat16)
        normed[span(i)] = rounded
        for t in range(tiles):
            cols = slice(t * tile, (t + 1) * tile)
            preact = jnp.dot(rounded, full[:, cols], preferred_element_type=jnp.float32)
            cdf = 0.5 * (1.0 + lax.erf(preact * half_root))
            pdf = jnp.exp(-0.5 * preact * preact) * density_scale
            deriv[span(i), cols] = cdf + preact * pdf
            outgoing[span(i), cols] = (values[:, cols] + preact * cdf).astype(jnp.bfloat16)

        @pl.when(section < last)
        def _():
            fwd_copy(i).start()

        terms[chip, span(i)] = normed[span(i), pl.ds(own_columns, 2 * shard_rows)]
        for k in range(1, chips):
            term_copy(k, i).start()

    lag = min(2, steps)

    def backward(i):
        @pl.when(section < last)
        def _():
            bwd_arrival(i).wait_recv()

        above = upstream[span(i)].astype(jnp.float32)
        grad_pre = (above * deriv[span(i)]).astype(jnp.bfloat16)
        grads[chip, span(i)] = grad_pre
        for h in HALVES:
            for way in (0, 1):
                grad_own(way, h if way == 0 else 1 - h, i).start()

        @pl.when(i >= lag)
        def _():
            pass_on(i - lag)

        @pl.when(section > 0)
        def _():
            values = hidden[span(i)].astype(jnp.float32)
            scale = lax.rsqrt(jnp.mean(values * values, axis=-1, keepdims=True) + epsilon)
            along = jnp.zeros((chunk, 1), jnp.float32)
            for t in range(tiles):
                cols = slice(t * tile, (t + 1) * tile)
                piece = lax.dot_general(
                    grad_pre, full[cols, :], (((1,), (1,)), ((), ())), preferred_element_type=jnp.float32
                ) * gain[:, cols]
                scaled[:, cols] = piece
                along = along + jnp.sum(piece * values[:, cols], axis=-1, keepdims=True)
            pull = scale * scale * scale * (along / width)
            result = upstream[span(i)].astype(jnp.float32) + scale * scaled[...] - values * pull
            downstream[span(i)] = result.astype(jnp.bfloat16)
            bwd_copy(i).start()

    def step(k, carry):
        at_last = (section == last).astype(jnp.int32)
        half = lax.div(k, 2)
        goes_back = at_last * lax.rem(k, 2) + (1 - at_last) * lax.div(k, steps)
        index = at_last * half + (1 - at_last) * lax.rem(k, steps)

        @pl.when(goes_back == 0)
        def _():
            forward(index)

        @pl.when(goes_back == 1)
        def _():
            backward(index)

        return carry

    lax.fori_loop(0, 2 * steps, step, 0)

    def arrivals(i, carry):
        for k in range(1, chips):
            source = peer_chip(k)
            remote(
                terms.at[source, span(i)], terms.at[source, span(i)],
                term_send.at[k, i], term_recv.at[source, i], at_dp(me),
            ).wait_recv()
        for way in (0, 1):
            grad_arrival(near[way], 1 - way, i).wait_recv()
        for h in HALVES:
            grad_arrival(corner, h, i).wait_recv()
        return carry

    for i in range(steps - lag, steps):
        pass_on(i)

    lax.fori_loop(0, steps, arrivals, 0)

    def product(half, cols):
        left = pl.ds(pl.multiple_of(half * shard_rows, shard_rows), shard_rows)
        total = jnp.zeros((shard_rows, tile), jnp.float32)
        for c in range(chips):
            total = total + lax.dot_general(
                terms[c, :, left], grads[c, :, cols], (((0,), (0,)), ((), ())), preferred_element_type=jnp.float32
            )
        return total

    def part_copy(t):
        return remote(partial.at[t], incoming.at[t], part_send.at[t], part_recv.at[t], at_dp(sibling))

    for t in range(tiles):
        partial[t] = product(1 - core, slice(t * tile, (t + 1) * tile)).astype(jnp.bfloat16)
        part_copy(t).start()
    own_rows = pl.ds(pl.multiple_of(me * shard_rows, shard_rows), shard_rows)
    for t in range(tiles):
        cols = slice(t * tile, (t + 1) * tile)
        pruned = weight[:, cols].astype(jnp.float32) - full[own_rows, cols].astype(jnp.float32)
        out[:, cols] = product(core, cols) * (1.0 / math.sqrt(tokens)) + decay_rate * pruned

    for k in range(1, chips):
        flip_copy(k, peer_chip(k)).wait_recv()
    total = counts[0]
    for c in range(1, chips):
        total = total + counts[c]
    counts[chips] = total
    pair_copy = remote(counts.at[chips], counts.at[chips + 1], pair_sem.at[0], pair_sem.at[1], at_dp(sibling))
    pair_copy.start()

    for t in range(tiles):
        cols = slice(t * tile, (t + 1) * tile)
        part_copy(t).wait_recv()
        out[:, cols] = out[:, cols] + incoming[t].astype(jnp.float32) * (1.0 / math.sqrt(tokens))
    pair_copy.wait_recv()
    flips[...] = counts[chips] + counts[chips + 1]

    pair_copy.wait_send()
    for t in range(tiles):
        part_copy(t).wait_send()
    for k in range(1, chips):
        flip_copy(k, chip).wait_send()

    for way in (0, 1):
        pack_onward(way).wait_send()
        for h in HALVES:
            pack_own(way, h).wait_send()
    for c in range(chips):
        relay_copy(c, core).wait_send()

    def drain(i, carry):
        for k in range(1, chips):
            term_copy(k, i).wait_send()
        for way in (0, 1):
            grad_onward(way, i).wait_send()
            for h in HALVES:
                grad_own(way, h, i).wait_send()

        @pl.when(section < last)
        def _():
            fwd_copy(i).wait_send()

        @pl.when(section > 0)
        def _():
            bwd_copy(i).wait_send()

        return carry

    lax.fori_loop(0, steps, drain, 0)


def fused_body(activations, cotangent, weight, norm_gain, pair_mask, earlier_mask):
    replicas = lax.axis_size("dp")
    chips = replicas // 2
    micro, micro_rows, width = activations.shape
    shard_rows = weight.shape[1]
    groups = shard_rows // 4
    rows = micro * micro_rows
    chunk = pick_chunk(rows)
    steps = rows // chunk
    tile = 512
    tiles = width // tile
    bf, f32 = jnp.bfloat16, jnp.float32
    dma = pltpu.SemaphoreType.DMA
    vmem = pl.BlockSpec(memory_space=pltpu.VMEM)
    hbm = pl.BlockSpec(memory_space=pl.ANY)
    gradient, flips = pl.pallas_call(
        functools.partial(fused_kernel, chunk, rows * replicas),
        out_shape=(
            jax.ShapeDtypeStruct((shard_rows, width), f32),
            jax.ShapeDtypeStruct((8, 128), jnp.int32),
        ),
        in_specs=[hbm, hbm, vmem, vmem, hbm, vmem],
        out_specs=(vmem, vmem),
        scratch_shapes=[
            pltpu.VMEM((replicas, 2 * groups, width), bf),
            pltpu.VMEM((width, width), bf),
            pltpu.VMEM((rows, width), bf),
            pltpu.VMEM((rows, width), bf),
            pltpu.VMEM((rows, width), f32),
            pltpu.VMEM((rows, width), bf),
            pltpu.VMEM((rows, width), bf),
            pltpu.VMEM((rows, width), bf),
            pltpu.VMEM((chips, rows, width), bf),
            pltpu.VMEM((chips, rows, 2 * shard_rows), bf),
            pltpu.VMEM((chunk, width), f32),
            pltpu.VMEM((tiles, shard_rows, tile), bf),
            pltpu.VMEM((tiles, shard_rows, tile), bf),
            pltpu.VMEM((chips + 2, 8, 128), jnp.int32),
            pltpu.VMEM((width // 4, width), jnp.int32),
            pltpu.VMEM((groups, width), jnp.int32),
            dma((2,)), dma((micro,)),
            dma((3, 2)), dma((chips, 2)), dma((chips,)), dma((chips,)),
            dma((steps,)), dma((steps,)), dma((steps,)), dma((steps,)),
            dma((chips, steps)), dma((chips, steps)), dma((6, steps)), dma((2 * chips, steps)),
            dma((tiles,)), dma((tiles,)), dma((chips,)), dma((chips,)), dma((2,)),
        ],
        compiler_params=pltpu.CompilerParams(
            collective_id=0, has_side_effects=True, vmem_limit_bytes=60 * 2**20
        ),
        name="fused_step",
    )(
        activations, cotangent, weight[0], norm_gain, pair_mask[0], earlier_mask[0],
    )
    return (gradient[None], jnp.sum(flips).reshape(1))


def solution(mesh):
    placed = (
        P(None, "dp", None),
        P(None, "dp", None),
        P("section", "dp", None),
        P("section", None),
        P("section", None, None),
        P("section", "dp", None),
    )

    def step(*arrays):
        chosen = fused_body if fused_fits(mesh, arrays[0], arrays[2]) else body
        return jax.shard_map(
            chosen,
            mesh=mesh,
            in_specs=placed,
            out_specs=(P("section", "dp", None), P("section")),
            check_vma=False,
        )(*arrays)

    return step
```

```python
import functools
import math

import jax
import jax.numpy as jnp
from jax import lax
from jax.experimental import pallas as pl
from jax.experimental.pallas import tpu as pltpu
from jax.sharding import PartitionSpec as P

epsilon = 1e-06
decay_rate = 4.0
half_root = 0.7071067811865476
density_scale = 0.3989422804014327
first_table = (0, 0, 0, 1, 1, 2)
second_table = (1, 2, 3, 2, 3, 3)


def shifted(block, axis, distance):
    devices = range(lax.axis_size(axis))
    route = [(i - distance, i) for i in devices if i - distance in devices]
    return lax.ppermute(block, axis, route)


def pair_ends(indices):
    leading = jnp.zeros_like(indices)
    trailing = jnp.zeros_like(indices)
    for pair_index in range(6):
        matches = indices == pair_index
        leading = jnp.where(matches, first_table[pair_index], leading)
        trailing = jnp.where(matches, second_table[pair_index], trailing)
    return (leading, trailing)


def kept_positions(indices):
    leading, trailing = pair_ends(indices)
    groups, columns = indices.shape
    positions = lax.broadcasted_iota(jnp.int32, (groups, 4, columns), 1)
    kept_mask = (positions == leading[:, None, :]) | (positions == trailing[:, None, :])
    return kept_mask.reshape(groups * 4, columns)


def section_forward(inputs, masked, gain_row):
    values = inputs.astype(jnp.float32)
    norm_scale = lax.rsqrt(jnp.mean(values * values, axis=-1, keepdims=True) + epsilon)
    normed = (values * norm_scale * gain_row).astype(jnp.bfloat16)
    preact = jnp.dot(normed, masked, preferred_element_type=jnp.float32)
    normal_cdf = 0.5 * (1.0 + lax.erf(preact * half_root))
    outputs = (values + preact * normal_cdf).astype(jnp.bfloat16)
    return (normed, preact, outputs)


def section_backward(inputs, preact, upstream, masked, gain_row):
    values = inputs.astype(jnp.float32)
    norm_scale = lax.rsqrt(jnp.mean(values * values, axis=-1, keepdims=True) + epsilon)
    normal_cdf = 0.5 * (1.0 + lax.erf(preact * half_root))
    normal_pdf = jnp.exp(-0.5 * preact * preact) * density_scale
    upstream_f = upstream.astype(jnp.float32)
    grad_pre = (upstream_f * (normal_cdf + preact * normal_pdf)).astype(jnp.bfloat16)
    grad_normed = lax.dot_general(
        grad_pre, masked, (((1,), (1,)), ((), ())), preferred_element_type=jnp.float32
    )
    scaled_grad = grad_normed * gain_row
    grad_input = norm_scale * scaled_grad - values * norm_scale**3 * jnp.mean(
        scaled_grad * values, axis=-1, keepdims=True
    )
    return (grad_pre, (upstream_f + grad_input).astype(jnp.bfloat16))


def write_slot(buffer, new_value, slot_index, is_live):
    old_value = lax.dynamic_index_in_dim(buffer, slot_index, 0, keepdims=False)
    chosen = jnp.where(is_live, new_value, old_value)
    return lax.dynamic_update_index_in_dim(buffer, chosen, slot_index, 0)


def body(activations, cotangent, weight, norm_gain, pair_mask, earlier_mask):
    section_count = lax.axis_size("section")
    replica_count = lax.axis_size("dp")
    section_index = lax.axis_index("section")
    replica_index = lax.axis_index("dp")
    micro_count, row_count, model_width = activations.shape
    shard_rows = weight.shape[1]
    groups = shard_rows // 4
    own_weight = weight[0]
    gain_row = norm_gain[0]
    own_pairs = lax.dynamic_slice_in_dim(pair_mask[0], replica_index * groups, groups, 0)
    own_kept = kept_positions(own_pairs)
    earlier_kept = kept_positions(earlier_mask[0])
    flip_local = jnp.sum(own_kept != earlier_kept).reshape(1)
    flip_sum = lax.psum(flip_local, "dp")
    masked_shard = jnp.where(own_kept, own_weight, jnp.zeros_like(own_weight))
    masked = lax.all_gather(masked_shard, "dp", axis=0, tiled=True)
    tick_count = micro_count + section_count - 1
    act_zeros = jnp.zeros((micro_count, row_count, model_width), jnp.bfloat16)
    stored = (act_zeros,)

    def forward_tick(tick_index, state_tuple):
        received, buffers = state_tuple
        micro_index = tick_index - section_index
        is_live = (micro_index >= 0) & (micro_index < micro_count)
        slot_index = jnp.clip(micro_index, 0, micro_count - 1)
        fresh_rows = lax.dynamic_index_in_dim(activations, slot_index, 0, keepdims=False)
        current = jnp.where(section_index == 0, fresh_rows, received)
        normed, preact, outputs = section_forward(current, masked, gain_row)
        results = (current, normed, preact)
        buffers = tuple(
            (
                write_slot(buffer, update, slot_index, is_live)
                for buffer, update in zip(buffers, results)
            )
        )
        received = shifted(outputs, "section", 1)
        return (received, buffers)

    start_rows = jnp.zeros((row_count, model_width), jnp.bfloat16)
    received, stored = lax.fori_loop(0, tick_count, forward_tick, (start_rows, stored))

    def backward_tick(tick_index, state_tuple):
        received, grad_buffer, normed_buffer = state_tuple
        micro_index = tick_index - (section_count - 1 - section_index)
        is_live = (micro_index >= 0) & (micro_index < micro_count)
        slot_index = jnp.clip(micro_index, 0, micro_count - 1)
        fresh_rows = lax.dynamic_index_in_dim(cotangent, slot_index, 0, keepdims=False)
        upstream = jnp.where(section_index == section_count - 1, fresh_rows, received)
        inputs = lax.dynamic_index_in_dim(stored[0], slot_index, 0, keepdims=False)
        normed, preact, unused = section_forward(inputs, masked, gain_row)
        normed_buffer = write_slot(normed_buffer, normed, slot_index, is_live)
        grad_pre, grad_input = section_backward(inputs, preact, upstream, masked, gain_row)
        grad_buffer = write_slot(grad_buffer, grad_pre, slot_index, is_live)
        received = shifted(grad_input, "section", -1)
        return (received, grad_buffer, normed_buffer)

    received, grad_buffer, normed_buffer = lax.fori_loop(
        0, tick_count, backward_tick, (start_rows, act_zeros, act_zeros)
    )
    flat_normed = normed_buffer.reshape(micro_count * row_count, model_width)
    flat_grad = grad_buffer.reshape(micro_count * row_count, model_width)
    summed = lax.psum_scatter(
        lax.dot_general(
            flat_normed, flat_grad, (((0,), (0,)), ((), ())), preferred_element_type=jnp.float32
        ).astype(jnp.bfloat16),
        "dp",
        scatter_dimension=0,
        tiled=True,
    ).astype(jnp.float32)
    token_total = micro_count * row_count * replica_count
    dense_part = summed / math.sqrt(token_total)
    decay_part = jnp.where(own_kept, 0.0, own_weight.astype(jnp.float32))
    gradient = dense_part + decay_rate * decay_part
    return (gradient[None], flip_sum)


HALVES = (0, 1)


def pick_chunk(rows):
    return 32 if rows % 32 == 0 else 16


def fused_fits(mesh, activations, weight):
    replicas, sections = mesh.shape["dp"], mesh.shape["section"]
    micro, batch, width = activations.shape
    shard_rows = weight.shape[1] // replicas
    rows = micro * batch // replicas
    gathered = replicas // 2 * rows * width * 2
    return (
        replicas % 2 == 0
        and replicas == 2 * len(HALVES) ** 2
        and sections > 1
        and shard_rows % 128 == 0
        and rows % 16 == 0
        and width % 512 == 0
        and gathered + 3 * width * width * 2 < 40 * 2**20
    )


def spread_matrix(count, transposed):
    groups = count // 4
    rows = lax.broadcasted_iota(jnp.int32, (count, count), 1 if transposed else 0)
    columns = lax.broadcasted_iota(jnp.int32, (count, count), 0 if transposed else 1)
    place = sum((columns >= groups * j).astype(jnp.int32) for j in (1, 2, 3))
    hit = rows == 4 * (columns - groups * place) + place
    return jnp.where(hit, 1.0, 0.0).astype(jnp.bfloat16)


def fused_kernel(
    chunk, tokens, act, cot, weight, gain, pairs_hbm, earlier, out, flips,
    packed, full, hidden, normed, deriv, outgoing, upstream, downstream, grads, terms,
    scaled, partial, incoming, counts, pairs, own_pairs, load_sem, row_sem, turned, result_tiles, out_sem,
    pack_send, pack_recv, relay_send, relay_recv, fwd_send, fwd_recv, bwd_send, bwd_recv,
    term_send, term_recv, grad_send, grad_recv, part_send, part_recv, flip_send, flip_recv, pair_sem,
):
    section = lax.axis_index("section")
    sections = lax.axis_size("section")
    me = lax.axis_index("dp")
    chips = lax.axis_size("dp") // 2
    chip = lax.div(me, 2)
    core = lax.rem(me, 2)
    sibling = 2 * chip + 1 - core
    last = sections - 1
    shard_rows, width = weight.shape
    groups = shard_rows // 4
    rows = hidden.shape[0]
    steps = rows // chunk
    tile = 512
    tiles = width // tile
    across = chip + 1 - 2 * lax.rem(chip, 2)
    along_y = lax.rem(chip + 2, chips)
    corner = lax.rem(across + 2, chips)
    near = (across, along_y)
    own_columns = pl.multiple_of(chip * 2 * shard_rows, 2 * shard_rows)

    def peer_chip(k):
        return lax.rem(chip + k, chips)

    def at_dp(index):
        return {"dp": index}

    def remote(src, dst, send, recv, where):
        return pltpu.make_async_remote_copy(
            src_ref=src, dst_ref=dst, send_sem=send, recv_sem=recv,
            device_id=where, device_id_type=pl.DeviceIdType.MESH,
        )

    barrier = pltpu.get_barrier_semaphore()

    def greet(where):
        pl.semaphore_signal(barrier, inc=1, device_id=where, device_id_type=pl.DeviceIdType.MESH)

    for k in range(1, chips):
        greet(at_dp(2 * peer_chip(k) + core))
    greet(at_dp(sibling))

    @pl.when(section > 0)
    def _():
        greet({"section": section - 1})

    @pl.when(section < last)
    def _():
        greet({"section": section + 1})

    own_load = pltpu.make_async_copy(
        pairs_hbm.at[pl.ds(pl.multiple_of(me * groups, groups), groups), :], own_pairs, load_sem.at[0]
    )
    own_load.start()
    all_load = pltpu.make_async_copy(pairs_hbm, pairs, load_sem.at[1])
    all_load.start()
    micro_rows = act.shape[1]

    def row_loads(source, target):
        return [
            pltpu.make_async_copy(source.at[m], target.at[pl.ds(m * micro_rows, micro_rows)], row_sem.at[m])
            for m in range(act.shape[0])
        ]

    @pl.when(section == 0)
    def _():
        for load in row_loads(act, hidden):
            load.start()

    @pl.when(section == last)
    def _():
        for load in row_loads(cot, upstream):
            load.start()

    own_load.wait()
    gather_rows = spread_matrix(shard_rows, True)
    for t in range(tiles):
        cols = slice(t * tile, (t + 1) * tile)
        split = jnp.dot(gather_rows, weight[:, cols], preferred_element_type=jnp.float32)
        w0, w1, w2, w3 = (split[j * groups:(j + 1) * groups] for j in range(4))
        p = own_pairs[:, cols]
        first = jnp.where(p <= 2, w0, jnp.where(p <= 4, w1, w2))
        second = jnp.where(p == 0, w1, jnp.where((p == 1) | (p == 3), w2, w3))
        packed[me, 0:groups, cols] = first.astype(jnp.bfloat16)
        packed[me, groups:2 * groups, cols] = second.astype(jnp.bfloat16)

    pl.semaphore_wait(barrier, chips + (section > 0).astype(jnp.int32) + (section < last).astype(jnp.int32))

    def half_rows(h):
        return pl.ds(h * groups, groups)

    def pack_copy(way, source, h, route):
        slot = packed.at[2 * source + core, half_rows(h)]
        return remote(slot, slot, pack_send.at[route, h], pack_recv.at[source, h], at_dp(2 * near[way] + core))

    def pack_own(way, h):
        return pack_copy(way, chip, h, way)

    def pack_onward(way):
        return pack_copy(1 - way, near[way], way, 2)

    def pack_arrival(source, h):
        return pack_copy(0, source, h, 0)

    def relay_copy(source, parity):
        slot = packed.at[2 * source + parity]
        return remote(slot, slot, relay_send.at[source], relay_recv.at[source], at_dp(sibling))

    for h in HALVES:
        for way in (0, 1):
            pack_own(way, h if way == 0 else 1 - h).start()
    relay_copy(chip, core).start()

    p = own_pairs[...]
    q = earlier[...]
    changed = jnp.where(p == q, 0, jnp.where(p + q == 5, 4, 2))
    total = jnp.zeros((8, 128), jnp.int32)
    for a in range(groups // 8):
        for b in range(width // 128):
            total = total + changed[a * 8:(a + 1) * 8, b * 128:(b + 1) * 128]
    counts[chip] = total

    def flip_copy(k, source):
        slot = counts.at[source]
        return remote(slot, slot, flip_send.at[k], flip_recv.at[source], at_dp(2 * peer_chip(k) + core))

    for k in range(1, chips):
        flip_copy(k, chip).start()

    spread_rows = spread_matrix(shard_rows, False)

    def unpack(owner):
        owned = pl.multiple_of(owner * groups, groups)
        target = pl.multiple_of(owner * shard_rows, shard_rows)
        for t in range(tiles):
            cols = slice(t * tile, (t + 1) * tile)
            p = pairs[pl.ds(owned, groups), cols]
            v0 = packed[owner, 0:groups, cols].astype(jnp.float32)
            v1 = packed[owner, groups:2 * groups, cols].astype(jnp.float32)
            zero = jnp.zeros_like(v0)
            parts = (
                jnp.where(p <= 2, v0, zero),
                jnp.where((p == 3) | (p == 4), v0, jnp.where(p == 0, v1, zero)),
                jnp.where(p == 5, v0, jnp.where((p == 1) | (p == 3), v1, zero)),
                jnp.where((p == 2) | (p >= 4), v1, zero),
            )
            stacked = jnp.concatenate(parts, axis=0).astype(jnp.bfloat16)
            spread = jnp.dot(spread_rows, stacked, preferred_element_type=jnp.float32)
            full[pl.ds(target, shard_rows), cols] = spread.astype(jnp.bfloat16)

    all_load.wait()

    def unpack_two(first, second):
        def one(k, carry):
            unpack(jnp.where(k == 0, first, second))
            return carry

        lax.fori_loop(0, 2, one, 0)

    relay_copy(chip, 1 - core).wait_recv()
    unpack_two(2 * chip + core, 2 * chip + 1 - core)
    for way in (0, 1):
        pack_arrival(near[way], way).wait_recv()
        pack_onward(way).start()
    for way in (0, 1):
        pack_arrival(near[way], 1 - way).wait_recv()
        relay_copy(near[way], core).start()
    unpack_two(2 * across + core, 2 * along_y + core)
    for way in (0, 1):
        relay_copy(near[way], 1 - core).wait_recv()
    unpack_two(2 * across + 1 - core, 2 * along_y + 1 - core)
    for h in HALVES:
        pack_arrival(corner, h).wait_recv()
    relay_copy(corner, core).start()
    unpack_two_first = 2 * corner + core
    relay_copy(corner, 1 - core).wait_recv()
    unpack_two(unpack_two_first, 2 * corner + 1 - core)

    @pl.when(section == 0)
    def _():
        for load in row_loads(act, hidden):
            load.wait()

    @pl.when(section == last)
    def _():
        for load in row_loads(cot, upstream):
            load.wait()

    @pl.when(section == last)
    def _():
        def turn(r, carry):
            block = pl.ds(pl.multiple_of(r * shard_rows, shard_rows), shard_rows)
            for t in range(tiles):
                cols = slice(t * tile, (t + 1) * tile)
                turned[cols, block] = full[block, cols].T
            return carry

        lax.fori_loop(0, 2 * chips, turn, 0)

    def span(i):
        return pl.ds(pl.multiple_of(i * chunk, chunk), chunk)

    def fwd_copy(i):
        return remote(outgoing.at[span(i)], hidden.at[span(i)], fwd_send.at[i], fwd_recv.at[i], {"section": section + 1})

    def fwd_arrival(i):
        return remote(outgoing.at[span(i)], hidden.at[span(i)], fwd_send.at[i], fwd_recv.at[i], {"section": section})

    def bwd_copy(i):
        return remote(downstream.at[span(i)], upstream.at[span(i)], bwd_send.at[i], bwd_recv.at[i], {"section": section - 1})

    def bwd_arrival(i):
        return remote(downstream.at[span(i)], upstream.at[span(i)], bwd_send.at[i], bwd_recv.at[i], {"section": section})

    def term_copy(k, i):
        peer = peer_chip(k)
        wanted = pl.ds(pl.multiple_of(peer * 2 * shard_rows, 2 * shard_rows), 2 * shard_rows)
        return remote(
            normed.at[span(i), wanted], terms.at[chip, span(i)],
            term_send.at[k, i], term_recv.at[chip, i], at_dp(2 * peer + core),
        )

    def grad_copy(way, source, h, route, i):
        slot = grads.at[source, span(i), pl.ds(h * (width // 2), width // 2)]
        return remote(
            slot, slot, grad_send.at[route * 2 + h, i], grad_recv.at[source * 2 + h, i], at_dp(2 * near[way] + core)
        )

    def grad_own(way, h, i):
        return grad_copy(way, chip, h, way, i)

    def grad_onward(way, i):
        return grad_copy(1 - way, near[way], way, 2, i)

    def grad_arrival(source, h, i):
        return grad_copy(0, source, h, 0, i)

    def pass_on(i):
        for way in (0, 1):
            grad_arrival(near[way], way, i).wait_recv()
            grad_onward(way, i).start()

    def forward(i):
        @pl.when(section > 0)
        def _():
            fwd_arrival(i).wait_recv()

        values = hidden[span(i)].astype(jnp.float32)
        scale = lax.rsqrt(jnp.mean(values * values, axis=-1, keepdims=True) + epsilon)
        rounded = (values * scale * gain[...]).astype(jnp.bfloat16)
        normed[span(i)] = rounded
        for t in range(tiles):
            cols = slice(t * tile, (t + 1) * tile)
            preact = jnp.dot(rounded, full[:, cols], preferred_element_type=jnp.float32)
            cdf = 0.5 * (1.0 + lax.erf(preact * half_root))
            pdf = jnp.exp(-0.5 * preact * preact) * density_scale
            deriv[span(i), cols] = cdf + preact * pdf
            outgoing[span(i), cols] = (values[:, cols] + preact * cdf).astype(jnp.bfloat16)

        @pl.when(section < last)
        def _():
            fwd_copy(i).start()

        terms[chip, span(i)] = normed[span(i), pl.ds(own_columns, 2 * shard_rows)]
        for k in range(1, chips):
            term_copy(k, i).start()

    lag = min(2, steps)

    def backward(i):
        @pl.when(section < last)
        def _():
            bwd_arrival(i).wait_recv()

        above = upstream[span(i)].astype(jnp.float32)
        grad_pre = (above * deriv[span(i)]).astype(jnp.bfloat16)
        grads[chip, span(i)] = grad_pre
        for h in HALVES:
            for way in (0, 1):
                grad_own(way, h if way == 0 else 1 - h, i).start()

        @pl.when(i >= lag)
        def _():
            pass_on(i - lag)

        @pl.when(section > 0)
        def _():
            values = hidden[span(i)].astype(jnp.float32)
            scale = lax.rsqrt(jnp.mean(values * values, axis=-1, keepdims=True) + epsilon)
            def pull_back(is_turned):
                for t in range(tiles):
                    cols = slice(t * tile, (t + 1) * tile)
                    if is_turned:
                        piece = jnp.dot(grad_pre, turned[:, cols], preferred_element_type=jnp.float32)
                    else:
                        piece = lax.dot_general(
                            grad_pre, full[cols, :], (((1,), (1,)), ((), ())), preferred_element_type=jnp.float32
                        )
                    scaled[:, cols] = piece * gain[:, cols]

            @pl.when(section == last)
            def _():
                pull_back(True)

            @pl.when(section < last)
            def _():
                pull_back(False)

            along = jnp.sum(scaled[...] * values, axis=-1, keepdims=True)
            pull = scale * scale * scale * (along / width)
            result = upstream[span(i)].astype(jnp.float32) + scale * scaled[...] - values * pull
            downstream[span(i)] = result.astype(jnp.bfloat16)
            bwd_copy(i).start()

    def step(k, carry):
        at_last = (section == last).astype(jnp.int32)
        half = lax.div(k, 2)
        goes_back = at_last * lax.rem(k, 2) + (1 - at_last) * lax.div(k, steps)
        index = at_last * half + (1 - at_last) * lax.rem(k, steps)

        @pl.when(goes_back == 0)
        def _():
            forward(index)

        @pl.when(goes_back == 1)
        def _():
            backward(index)

        return carry

    lax.fori_loop(0, 2 * steps, step, 0)

    def arrivals(i, carry):
        for k in range(1, chips):
            source = peer_chip(k)
            remote(
                terms.at[source, span(i)], terms.at[source, span(i)],
                term_send.at[k, i], term_recv.at[source, i], at_dp(me),
            ).wait_recv()
        for way in (0, 1):
            grad_arrival(near[way], 1 - way, i).wait_recv()
        for h in HALVES:
            grad_arrival(corner, h, i).wait_recv()
        return carry

    for i in range(steps - lag, steps):
        pass_on(i)

    lax.fori_loop(0, steps, arrivals, 0)

    def product(half, cols):
        left = pl.ds(pl.multiple_of(half * shard_rows, shard_rows), shard_rows)
        total = jnp.zeros((shard_rows, tile), jnp.float32)
        for c in range(chips):
            total = total + lax.dot_general(
                terms[c, :, left], grads[c, :, cols], (((0,), (0,)), ((), ())), preferred_element_type=jnp.float32
            )
        return total

    def out_copy(t):
        return pltpu.make_async_copy(result_tiles.at[t], out.at[:, pl.ds(t * tile, tile)], out_sem.at[t])

    def part_copy(t):
        return remote(partial.at[t], incoming.at[t], part_send.at[t], part_recv.at[t], at_dp(sibling))

    for t in range(tiles):
        partial[t] = product(1 - core, slice(t * tile, (t + 1) * tile)).astype(jnp.bfloat16)
        part_copy(t).start()
    own_rows = pl.ds(pl.multiple_of(me * shard_rows, shard_rows), shard_rows)
    for t in range(tiles):
        cols = slice(t * tile, (t + 1) * tile)
        pruned = weight[:, cols].astype(jnp.float32) - full[own_rows, cols].astype(jnp.float32)
        result_tiles[t] = product(core, cols) * (1.0 / math.sqrt(tokens)) + decay_rate * pruned

    for k in range(1, chips):
        flip_copy(k, peer_chip(k)).wait_recv()
    total = counts[0]
    for c in range(1, chips):
        total = total + counts[c]
    counts[chips] = total
    pair_copy = remote(counts.at[chips], counts.at[chips + 1], pair_sem.at[0], pair_sem.at[1], at_dp(sibling))
    pair_copy.start()

    for t in range(tiles):
        cols = slice(t * tile, (t + 1) * tile)
        part_copy(t).wait_recv()
        result_tiles[t] = result_tiles[t] + incoming[t].astype(jnp.float32) * (1.0 / math.sqrt(tokens))
        out_copy(t).start()
    pair_copy.wait_recv()
    flips[...] = counts[chips] + counts[chips + 1]

    pair_copy.wait_send()
    for t in range(tiles):
        part_copy(t).wait_send()
    for k in range(1, chips):
        flip_copy(k, chip).wait_send()

    for way in (0, 1):
        pack_onward(way).wait_send()
        for h in HALVES:
            pack_own(way, h).wait_send()
    for c in range(chips):
        relay_copy(c, core).wait_send()

    def drain(i, carry):
        for k in range(1, chips):
            term_copy(k, i).wait_send()
        for way in (0, 1):
            grad_onward(way, i).wait_send()
            for h in HALVES:
                grad_own(way, h, i).wait_send()

        @pl.when(section < last)
        def _():
            fwd_copy(i).wait_send()

        @pl.when(section > 0)
        def _():
            bwd_copy(i).wait_send()

        return carry

    lax.fori_loop(0, steps, drain, 0)
    for t in range(tiles):
        out_copy(t).wait()


def fused_body(activations, cotangent, weight, norm_gain, pair_mask, earlier_mask):
    replicas = lax.axis_size("dp")
    chips = replicas // 2
    micro, micro_rows, width = activations.shape
    shard_rows = weight.shape[1]
    groups = shard_rows // 4
    rows = micro * micro_rows
    chunk = pick_chunk(rows)
    steps = rows // chunk
    tile = 512
    tiles = width // tile
    bf, f32 = jnp.bfloat16, jnp.float32
    dma = pltpu.SemaphoreType.DMA
    vmem = pl.BlockSpec(memory_space=pltpu.VMEM)
    hbm = pl.BlockSpec(memory_space=pl.ANY)
    gradient, flips = pl.pallas_call(
        functools.partial(fused_kernel, chunk, rows * replicas),
        out_shape=(
            jax.ShapeDtypeStruct((shard_rows, width), f32),
            jax.ShapeDtypeStruct((8, 128), jnp.int32),
        ),
        in_specs=[hbm, hbm, vmem, vmem, hbm, vmem],
        out_specs=(hbm, vmem),
        scratch_shapes=[
            pltpu.VMEM((replicas, 2 * groups, width), bf),
            pltpu.VMEM((width, width), bf),
            pltpu.VMEM((rows, width), bf),
            pltpu.VMEM((rows, width), bf),
            pltpu.VMEM((rows, width), f32),
            pltpu.VMEM((rows, width), bf),
            pltpu.VMEM((rows, width), bf),
            pltpu.VMEM((rows, width), bf),
            pltpu.VMEM((chips, rows, width), bf),
            pltpu.VMEM((chips, rows, 2 * shard_rows), bf),
            pltpu.VMEM((chunk, width), f32),
            pltpu.VMEM((tiles, shard_rows, tile), bf),
            pltpu.VMEM((tiles, shard_rows, tile), bf),
            pltpu.VMEM((chips + 2, 8, 128), jnp.int32),
            pltpu.VMEM((width // 4, width), jnp.int32),
            pltpu.VMEM((groups, width), jnp.int32),
            dma((2,)), dma((micro,)),
            pltpu.VMEM((width, width), bf),
            pltpu.VMEM((tiles, shard_rows, tile), f32),
            dma((tiles,)),
            dma((3, 2)), dma((chips, 2)), dma((chips,)), dma((chips,)),
            dma((steps,)), dma((steps,)), dma((steps,)), dma((steps,)),
            dma((chips, steps)), dma((chips, steps)), dma((6, steps)), dma((2 * chips, steps)),
            dma((tiles,)), dma((tiles,)), dma((chips,)), dma((chips,)), dma((2,)),
        ],
        compiler_params=pltpu.CompilerParams(
            collective_id=0, has_side_effects=True, vmem_limit_bytes=60 * 2**20
        ),
        name="fused_step",
    )(
        activations, cotangent, weight[0], norm_gain, pair_mask[0], earlier_mask[0],
    )
    return (gradient[None], jnp.sum(flips).reshape(1))


def solution(mesh):
    placed = (
        P(None, "dp", None),
        P(None, "dp", None),
        P("section", "dp", None),
        P("section", None),
        P("section", None, None),
        P("section", "dp", None),
    )

    def step(*arrays):
        chosen = fused_body if fused_fits(mesh, arrays[0], arrays[2]) else body
        return jax.shard_map(
            chosen,
            mesh=mesh,
            in_specs=placed,
            out_specs=(P("section", "dp", None), P("section")),
            check_vma=False,
        )(*arrays)

    return step
```
